32 devices in a mesh: groups: 2 (over x), blk: 16 (over z, y, core).
Axes of the slice: x: 2, y: 2, z: 4, core: 2. Of those that a mesh axis runs over, the one named last changes fastest.
Arguments:
- snapshots: bfloat16 [2, 65536, 2, 64], P('groups', 'blk'), parts along dimension 0, may hold values from -6 to 6
- bin_index: int32 [2], P('groups'), parts along dimension 0, may hold values from 1 to 4095
- positions: int32 [3, 65536], replicated, may hold values from 0 to 511
- directions: int32 [3, 4096], replicated, may hold values from -128 to 127
- taper: float32 [65536], replicated, may hold values from 0.5 to 2
- beam_order: int32 [4096], replicated, may hold values from 0 to 4095, each once
Outputs:
- beams: bfloat16 [4096, 2, 2, 64], P('blk', 'groups'), parts along dimension 1
The draws below stay inside these ranges and needn't reach their ends.
There are 2 independent parts, one for each index of `groups`. The reference program is written for one: setup_inputs(seed, part) draws one part's arguments, and reference() takes and returns one part's arrays. A program takes and returns all parts, laid end to end along the dimension named above; an argument that names none is the same for every part. Nothing has to cross between parts.
Inputs may be any that keep to these rules, and one draw needn't show every extreme that they name: beam_order is a permutation of the 4096 beams.
All inputs are finite; a program needn't handle non-finite values.
Results may differ from the reference program's by a relative error of at most 0.0048.
Values may be sent and summed in bfloat16 or wider, within the bound.
A program may use at most 64 MiB of HBM per device.

```python
import math
import jax
import jax.numpy as jnp
from jax import lax

ELEM = 65536
BEAMS = 4096
SNAP = 64
BINS = 1
CYCLE = 8192


def set_ends(entries, stream_key, low, top_value):
    shape = entries.shape
    spot = [jax.random.randint(jax.random.fold_in(stream_key, axis), (), 0, shape[axis]) for axis in range(len(shape))]
    entries = entries.at[tuple(spot)].set(low)
    longest = shape.index(max(shape))
    spot[longest] = (spot[longest] + 1) % shape[longest]
    return entries.at[tuple(spot)].set(top_value)


def block_levels(stream_key, extent, cuts, smallest, top_value):
    gain = 1.0
    for axis_at, parts in cuts:
        draws = jax.random.uniform(jax.random.fold_in(jax.random.fold_in(stream_key, 6), axis_at), (parts,), jnp.float32, smallest / len(cuts), top_value / len(cuts))
        gain = gain * jnp.repeat(jnp.exp(draws), extent[axis_at] // parts).reshape((-1,) + (1,) * (len(extent) - 1 - axis_at))
    return gain


def centred(own_key, dims, spread, most, pieces=(), held_as=jnp.bfloat16):
    drawn = spread * jax.random.normal(own_key, dims, jnp.float32)
    if pieces:
        drawn = drawn * block_levels(own_key, dims, pieces, -0.22, 0.18)
    return jnp.clip(drawn, -most, most).astype(held_as)


def setup_inputs(seed: int = 0, part: int = 0) -> dict:
    seeds = jax.random.split(jax.random.key(seed), 7)
    own_keys = jax.random.split(jax.random.fold_in(seeds[6], part), 7)
    snapshots = centred(own_keys[0], (BINS, ELEM, 2, SNAP), 1.0, 6.0, ((1, 16),))
    bin_index = jax.random.randint(own_keys[1], (BINS,), 1, CYCLE // 2).astype(jnp.int32)
    positions = set_ends(jax.random.randint(seeds[2], (3, ELEM), 0, 512), jax.random.fold_in(seeds[2], 1), 0, 511).astype(jnp.int32)
    directions = set_ends(jax.random.randint(seeds[3], (3, BEAMS), -128, 128), jax.random.fold_in(seeds[3], 1), -128, 127).astype(jnp.int32)
    taper = jnp.clip(jnp.exp(jax.random.uniform(seeds[4], (ELEM,), jnp.float32, math.log(0.5), math.log(2.0))), 0.5, 2.0)
    beam_order = jax.random.permutation(seeds[5], BEAMS).astype(jnp.int32)
    return dict(snapshots=snapshots, bin_index=bin_index, positions=positions, directions=directions, taper=taper, beam_order=beam_order)


def weight_block(dir_cols, positions, taper, bin_value):
    delays = dir_cols[0][:, None] * positions[0][None, :]
    delays = delays + dir_cols[1][:, None] * positions[1][None, :]
    delays = delays + dir_cols[2][:, None] * positions[2][None, :]
    delays = jnp.remainder(delays, CYCLE)
    phases = jnp.remainder(bin_value * delays, CYCLE)
    angles = phases.astype(jnp.float32) * (2.0 * math.pi / CYCLE)
    amplitude = (taper / math.sqrt(ELEM)).astype(jnp.float32)
    weight_re = (amplitude[None, :] * jnp.cos(angles)).astype(jnp.bfloat16)
    weight_im = (-amplitude[None, :] * jnp.sin(angles)).astype(jnp.bfloat16)
    return (weight_re, weight_im)

def beam_terms(dir_cols, positions, taper, snaps, bin_index):
    results = []
    for index in range(snaps.shape[0]):
        weight_re, weight_im = weight_block(dir_cols, positions, taper, bin_index[index])
        width = snaps.shape[3]
        columns = snaps[index].reshape(snaps.shape[1], 2 * width)
        with_real = jnp.dot(weight_re, columns, preferred_element_type=jnp.float32)
        with_imag = jnp.dot(weight_im, columns, preferred_element_type=jnp.float32)
        real_part = with_real[:, :width] - with_imag[:, width:]
        imag_part = with_real[:, width:] + with_imag[:, :width]
        results.append(jnp.stack([real_part, imag_part], axis=1))
    return jnp.stack(results, axis=1)

def reference(snapshots, bin_index, positions, directions, taper, beam_order):
    ordered = jnp.take(directions, beam_order, axis=1)
    row_block = math.gcd(BEAMS, 256)
    blocks = ordered.reshape(3, BEAMS // row_block, row_block).transpose(1, 0, 2)

    def per_block(dir_cols):
        return beam_terms(dir_cols, positions, taper, snapshots, bin_index)
    result = lax.map(per_block, blocks)
    return result.reshape(BEAMS, BINS, 2, SNAP).astype(jnp.bfloat16)
```

```python
import functools
import math

import jax
import jax.numpy as jnp
from jax import lax
from jax.experimental import pallas as pl
from jax.experimental.pallas import tpu as pltpu
from jax.sharding import PartitionSpec as P

CYCLE = 8192
FEATURES = 128
CENTRE = 256
DIGIT = 64
MAGIC = 1.5 * 2.0**23

SINE = (4.440887881768876, -7.256453678610621, 3.2286686850204496)
COSINE = (1.414177779756007, -6.976808749845299, 5.708615924866348, -1.7132819288833234)


def horner(coefficients, u):
    value = coefficients[-1] * u + coefficients[-2]
    for coefficient in coefficients[-3::-1]:
        value = value * u + coefficient
    return value


def cos_sin(cycles):
    nearest = (cycles + MAGIC) - MAGIC
    r = cycles - nearest
    u = r * r
    half_sine = r * horner(SINE, u)
    half_cosine = horner(COSINE, u)
    return 1.0 - half_sine * half_sine, half_sine * half_cosine


def kernel(
    n, tile_b, tile_e,
    feat_ref, pos_ref, with_cos_ref, with_sin_ref, out_ref,
    phase, wcos, wsin, acc, sendbuf, recv, send_sem, recv_sem,
):
    me = lax.axis_index("blk")
    owned = out_ref.shape[0]
    beams, local = feat_ref.shape[0], pos_ref.shape[1]
    per_block = tile_b // owned
    blocks, tiles = beams // tile_b, local // tile_e
    home = me // per_block

    barrier = pltpu.get_barrier_semaphore()

    @pl.loop(1, n)
    def _(k):
        pl.semaphore_signal(
            barrier, inc=1, device_id={"blk": lax.rem(me + k, n)},
            device_id_type=pl.DeviceIdType.MESH,
        )

    def block_at(j):
        return lax.rem(home + 1 + j, blocks)

    def phase_dot(j, tile, slot):
        rows = pl.multiple_of(block_at(j) * tile_b, tile_b)
        columns = pl.multiple_of(tile * tile_e, tile_e)
        phase[slot] = jnp.dot(
            feat_ref[pl.ds(rows, tile_b), :], pos_ref[:, pl.ds(columns, tile_e)],
            preferred_element_type=jnp.float32,
        )

    def trig(slot):
        rows, columns = 32, 256
        for c in range(0, tile_e, columns):
            for r in range(0, tile_b, rows):
                cosine, sine = cos_sin(phase[slot, r:r + rows, c:c + columns])
                wcos[slot, r:r + rows, c:c + columns] = cosine.astype(jnp.bfloat16)
                wsin[slot, r:r + rows, c:c + columns] = sine.astype(jnp.bfloat16)

    def main_dot(tile, slot, acc_slot, first):
        at = pl.ds(pl.multiple_of(tile * tile_e, tile_e), tile_e)
        total = jnp.dot(wcos[slot], with_cos_ref[at, :], preferred_element_type=jnp.float32)
        total += jnp.dot(wsin[slot], with_sin_ref[at, :], preferred_element_type=jnp.float32)
        acc[acc_slot] = total if first else acc[acc_slot] + total

    def copy_to(owner):
        return pltpu.make_async_remote_copy(
            src_ref=sendbuf.at[pl.ds(pl.multiple_of(owner * owned, owned), owned), :],
            dst_ref=recv.at[me],
            send_sem=send_sem.at[owner],
            recv_sem=recv_sem.at[me],
            device_id={"blk": owner},
            device_id_type=pl.DeviceIdType.MESH,
        )

    def finish(j):
        block = block_at(j)
        rows = pl.multiple_of(block * tile_b, tile_b)
        sendbuf[pl.ds(rows, tile_b), :] = acc[lax.rem(j, 2)].astype(jnp.bfloat16)
        for k in range(per_block):
            owner = block * per_block + k

            @pl.when(owner != me)
            def _():
                copy_to(owner).start()

    wcos[1] = jnp.zeros_like(wcos[1])
    wsin[1] = jnp.zeros_like(wsin[1])
    acc[1] = jnp.zeros_like(acc[1])
    phase_dot(0, 0, 0)

    @pl.loop(0, blocks)
    def _(j):
        here, there = lax.rem(j, 2), lax.rem(j + 1, 2)
        phase_dot(j, 1, 1)
        trig(0)
        main_dot(tiles - 1, 1, there, False)
        if tiles > 2:
            phase_dot(j, 2, 0)
        else:
            phase_dot(j + 1, 0, 0)
        trig(1)
        main_dot(0, 0, here, True)

        @pl.when(j == 1)
        def _():
            pl.semaphore_wait(barrier, n - 1)

        @pl.when(j > 0)
        def _():
            finish(j - 1)

        @pl.loop(1, tiles // 2)
        def _(i):
            phase_dot(j, 2 * i + 1, 1)
            trig(0)
            main_dot(2 * i - 1, 1, here, False)
            last = (2 * i + 2 == tiles).astype(jnp.int32)
            phase_dot(j + last, (2 * i + 2) * (1 - last), 0)
            trig(1)
            main_dot(2 * i, 0, here, False)

    last_slot = (blocks - 1) % 2
    main_dot(tiles - 1, 1, last_slot, False)
    if blocks == 1:
        pl.semaphore_wait(barrier, n - 1)
    finish(blocks - 1)

    own = pl.multiple_of((me - home * per_block) * owned, owned)
    out_total = acc.at[last_slot]

    @pl.loop(1, n)
    def _(k):
        sender = lax.rem(me + n - k, n)
        pltpu.make_async_remote_copy(
            src_ref=sendbuf.at[pl.ds(0, owned), :],
            dst_ref=recv.at[sender],
            send_sem=send_sem.at[sender],
            recv_sem=recv_sem.at[sender],
            device_id={"blk": sender},
            device_id_type=pl.DeviceIdType.MESH,
        ).wait()
        at = pl.ds(own, owned)
        out_total[at, :] = out_total[at, :] + recv[sender].astype(jnp.float32)

    out_ref[...] = out_total[pl.ds(own, owned), :].astype(jnp.bfloat16)


def per_device(snapshots, bin_index, positions, directions, taper, beam_order):
    n = lax.axis_size("blk")
    _, local, parts, width = snapshots.shape
    elements, beams = positions.shape[1], directions.shape[1]
    owned = beams // n
    tile_b, tile_e = min(512, beams), min(512, local // 2)

    offset = lax.axis_index("blk") * local
    local_positions = lax.dynamic_slice_in_dim(positions, offset, local, 1)
    local_taper = lax.dynamic_slice_in_dim(taper, offset, local, 0)

    steps = jnp.take(directions, beam_order, axis=1) * bin_index[0]
    steps = ((steps + CYCLE // 2) & (CYCLE - 1)) - CYCLE // 2
    low = steps & (DIGIT - 1)
    high = steps - low
    shift = (jnp.sum(steps, axis=0, keepdims=True) * CENTRE) & (CYCLE - 1)
    features = jnp.concatenate([high, low, shift], axis=0).astype(jnp.float32) / CYCLE
    features = jnp.pad(features.astype(jnp.bfloat16), ((0, FEATURES - 7), (0, 0))).T
    centred = local_positions - CENTRE
    points = jnp.concatenate([centred, centred, jnp.ones_like(centred[:1])], axis=0)
    points = jnp.pad(points.astype(jnp.bfloat16), ((0, FEATURES - 7), (0, 0)))

    amplitude = (local_taper / math.sqrt(elements))[:, None]
    real = (snapshots[0, :, 0, :] * amplitude).astype(jnp.bfloat16)
    imag = (snapshots[0, :, 1, :] * amplitude).astype(jnp.bfloat16)
    with_cos = jnp.concatenate([real, imag], axis=1)
    with_sin = jnp.concatenate([imag, -real], axis=1)

    columns = parts * width
    vmem = pl.BlockSpec(memory_space=pltpu.VMEM)
    result = pl.pallas_call(
        functools.partial(kernel, n, tile_b, tile_e),
        out_shape=jax.ShapeDtypeStruct((owned, columns), jnp.bfloat16),
        in_specs=[vmem] * 4,
        out_specs=vmem,
        scratch_shapes=[
            pltpu.VMEM((2, tile_b, tile_e), jnp.float32),
            pltpu.VMEM((2, tile_b, tile_e), jnp.bfloat16),
            pltpu.VMEM((2, tile_b, tile_e), jnp.bfloat16),
            pltpu.VMEM((2, tile_b, columns), jnp.float32),
            pltpu.VMEM((beams, columns), jnp.bfloat16),
            pltpu.VMEM((n, owned, columns), jnp.bfloat16),
            pltpu.SemaphoreType.DMA((n,)),
            pltpu.SemaphoreType.DMA((n,)),
        ],
        compiler_params=pltpu.CompilerParams(collective_id=0, has_side_effects=True),
    )(features, points, with_cos, with_sin)
    return result.reshape(owned, 1, parts, width)


def solution(mesh):
    in_specs = (P("groups", "blk", None, None), P("groups"), P(), P(), P(), P())
    out_specs = P("blk", "groups", None, None)
    return jax.shard_map(
        per_device, mesh=mesh, in_specs=in_specs, out_specs=out_specs, check_vma=False
    )
```

```python
import functools
import math

import jax
import jax.numpy as jnp
from jax import lax
from jax.experimental import pallas as pl
from jax.experimental.pallas import tpu as pltpu
from jax.sharding import PartitionSpec as P

CYCLE = 8192
FEATURES = 128
LANES = 128
CENTRE = 256
DIGIT = 64

SINE = (4.440887881768876, -7.256453678610621, 3.2286686850204496)
COSINE = (1.414177779756007, -6.976808749845299, 5.708615924866348, -1.7132819288833234)


def horner(coefficients, u):
    value = coefficients[-1] * u + coefficients[-2]
    for coefficient in coefficients[-3::-1]:
        value = value * u + coefficient
    return value


def cos_sin(cycles):
    nearest = jnp.round(cycles)
    r = cycles - nearest
    u = r * r
    half_sine = r * horner(SINE, u)
    half_cosine = horner(COSINE, u)
    return 1.0 - half_sine * half_sine, half_sine * half_cosine


def dot_rows(a, b):
    return lax.dot_general(a, b, (((1,), (1,)), ((), ())), preferred_element_type=jnp.float32)


def build_features(bin_value, direction_ref, order_ref, table, feat_ref):
    beams = direction_ref.shape[1]
    groups = beams // LANES
    table[...] = jnp.zeros_like(table)
    for h in range(groups):
        columns = direction_ref[:, h * LANES:(h + 1) * LANES].astype(jnp.float32)
        table[8 * h:8 * h + 3, :] = columns
    chunk = min(512, beams)

    @pl.loop(0, beams // chunk)
    def _(i):
        at = pl.ds(pl.multiple_of(i * chunk, chunk), chunk)
        order = order_ref[:, at]
        row = lax.broadcasted_iota(jnp.int32, (LANES, chunk), 0)
        hot = jnp.where(row == (order & (LANES - 1)), 1.0, 0.0).astype(jnp.bfloat16)
        picked = jnp.dot(table[...].astype(jnp.bfloat16), hot, preferred_element_type=jnp.float32)
        block = jnp.broadcast_to(order // LANES, (8, chunk))
        ordered = jnp.zeros((8, chunk), jnp.float32)
        for h in range(groups):
            ordered = jnp.where(block == h, picked[8 * h:8 * h + 8, :], ordered)
        steps = ordered.astype(jnp.int32) * bin_value
        steps = ((steps + CYCLE // 2) & (CYCLE - 1)) - CYCLE // 2
        low = steps & (DIGIT - 1)
        high = steps - low
        shift = ((steps[0:1] + steps[1:2] + steps[2:3]) * CENTRE) & (CYCLE - 1)
        row = lax.broadcasted_iota(jnp.int32, (8, chunk), 0)
        high = jnp.where(row == 3, jnp.broadcast_to(shift, (8, chunk)), high)
        zeros = jnp.zeros((FEATURES - 16, chunk), jnp.float32)
        scale = 1.0 / CYCLE
        features = jnp.concatenate(
            [high.astype(jnp.float32) * scale, low.astype(jnp.float32) * scale, zeros], axis=0
        )
        feat_ref[at, :] = features.T.astype(jnp.bfloat16)


def build_points(position_ref, raised, pos_ref):
    raised[...] = jnp.zeros_like(raised)
    raised[0:3, :] = (position_ref[...] - CENTRE).astype(jnp.float32)
    raised[3:4, :] = jnp.ones((1, raised.shape[1]), jnp.float32)
    pos_ref[...] = jnp.zeros_like(pos_ref)
    pos_ref[0:16, :] = jnp.concatenate([raised[...], raised[...]], axis=0).astype(jnp.bfloat16)


def scale_snapshots(scale, snap_ref, taper_ref, with_cos_ref, with_sin_ref):
    width, local = snap_ref.shape[0] // 2, snap_ref.shape[1]
    chunk = min(512, local)

    @pl.loop(0, local // chunk)
    def _(i):
        at = pl.ds(pl.multiple_of(i * chunk, chunk), chunk)
        amplitude = jnp.broadcast_to(taper_ref[:, at] * scale, (width, chunk))
        real = snap_ref[0:width, at].astype(jnp.float32) * amplitude
        imag = snap_ref[width:2 * width, at].astype(jnp.float32) * amplitude
        with_cos_ref[0:width, at] = real.astype(jnp.bfloat16)
        with_cos_ref[width:2 * width, at] = imag.astype(jnp.bfloat16)
        with_sin_ref[0:width, at] = imag.astype(jnp.bfloat16)
        with_sin_ref[width:2 * width, at] = (-real).astype(jnp.bfloat16)


def kernel(
    n, tile_b, tile_e,
    bin_ref, snap_ref, position_hbm, direction_ref, taper_hbm, order_ref, out_ref,
    position_ref, taper_ref, raised, table, feat_ref, pos_ref, with_cos_ref, with_sin_ref,
    phase, wcos, wsin, acc, sendbuf, recv, final, copy_sem, send_sem, recv_sem,
):
    me = lax.axis_index("blk")
    owned = out_ref.shape[1]
    beams, local = feat_ref.shape[0], pos_ref.shape[1]
    per_block = tile_b // owned
    blocks, tiles = beams // tile_b, local // tile_e
    home = me // per_block

    mine = pl.ds(pl.multiple_of(me * local, local), local)
    fetch_positions = pltpu.make_async_copy(position_hbm.at[:, mine], position_ref, copy_sem.at[0])
    fetch_taper = pltpu.make_async_copy(taper_hbm.at[:, mine], taper_ref, copy_sem.at[1])
    fetch_positions.start()
    fetch_taper.start()

    barrier = pltpu.get_barrier_semaphore()

    @pl.loop(1, n)
    def _(k):
        pl.semaphore_signal(
            barrier, inc=1, device_id={"blk": lax.rem(me + k, n)},
            device_id_type=pl.DeviceIdType.MESH,
        )

    build_features(bin_ref[0], direction_ref, order_ref, table, feat_ref)
    fetch_positions.wait()
    build_points(position_ref, raised, pos_ref)
    fetch_taper.wait()
    scale = 1.0 / math.sqrt(position_hbm.shape[1])
    scale_snapshots(scale, snap_ref, taper_ref, with_cos_ref, with_sin_ref)

    def block_at(j):
        return lax.rem(home + 1 + j, blocks)

    def phase_dot(j, tile, slot):
        rows = pl.multiple_of(block_at(j) * tile_b, tile_b)
        columns = pl.multiple_of(tile * tile_e, tile_e)
        phase[slot] = jnp.dot(
            feat_ref[pl.ds(rows, tile_b), :], pos_ref[:, pl.ds(columns, tile_e)],
            preferred_element_type=jnp.float32,
        )

    def trig(slot):
        rows, columns = 32, 256
        for c in range(0, tile_e, columns):
            for r in range(0, tile_b, rows):
                cosine, sine = cos_sin(phase[slot, r:r + rows, c:c + columns])
                wcos[slot, r:r + rows, c:c + columns] = cosine.astype(jnp.bfloat16)
                wsin[slot, r:r + rows, c:c + columns] = sine.astype(jnp.bfloat16)

    def main_dot(tile, slot, acc_slot, first):
        at = pl.ds(pl.multiple_of(tile * tile_e, tile_e), tile_e)
        total = dot_rows(wcos[slot], with_cos_ref[:, at])
        total += dot_rows(wsin[slot], with_sin_ref[:, at])
        acc[acc_slot] = total if first else acc[acc_slot] + total

    def copy_to(owner):
        return pltpu.make_async_remote_copy(
            src_ref=sendbuf.at[pl.ds(pl.multiple_of(owner * owned, owned), owned), :],
            dst_ref=recv.at[me],
            send_sem=send_sem.at[owner],
            recv_sem=recv_sem.at[me],
            device_id={"blk": owner},
            device_id_type=pl.DeviceIdType.MESH,
        )

    def finish(j):
        block = block_at(j)
        rows = pl.multiple_of(block * tile_b, tile_b)
        sendbuf[pl.ds(rows, tile_b), :] = acc[lax.rem(j, 2)].astype(jnp.bfloat16)
        for k in range(per_block):
            owner = block * per_block + k

            @pl.when(owner != me)
            def _():
                copy_to(owner).start()

    wcos[1] = jnp.zeros_like(wcos[1])
    wsin[1] = jnp.zeros_like(wsin[1])
    acc[1] = jnp.zeros_like(acc[1])
    phase_dot(0, 0, 0)

    @pl.loop(0, blocks)
    def _(j):
        here, there = lax.rem(j, 2), lax.rem(j + 1, 2)
        phase_dot(j, 1, 1)
        trig(0)
        main_dot(tiles - 1, 1, there, False)
        if tiles > 2:
            phase_dot(j, 2, 0)
        else:
            phase_dot(j + 1, 0, 0)
        trig(1)
        main_dot(0, 0, here, True)

        @pl.when(j == 1)
        def _():
            pl.semaphore_wait(barrier, n - 1)

        @pl.when(j > 0)
        def _():
            finish(j - 1)

        @pl.loop(1, tiles // 2)
        def _(i):
            phase_dot(j, 2 * i + 1, 1)
            trig(0)
            main_dot(2 * i - 1, 1, here, False)
            last = (2 * i + 2 == tiles).astype(jnp.int32)
            phase_dot(j + last, (2 * i + 2) * (1 - last), 0)
            trig(1)
            main_dot(2 * i, 0, here, False)

    last_slot = (blocks - 1) % 2
    main_dot(tiles - 1, 1, last_slot, False)
    if blocks == 1:
        pl.semaphore_wait(barrier, n - 1)
    finish(blocks - 1)

    own = pl.multiple_of((me - home * per_block) * owned, owned)
    out_total = acc.at[last_slot]

    @pl.loop(1, n)
    def _(k):
        sender = lax.rem(me + n - k, n)
        pltpu.make_async_remote_copy(
            src_ref=sendbuf.at[pl.ds(0, owned), :],
            dst_ref=recv.at[sender],
            send_sem=send_sem.at[sender],
            recv_sem=recv_sem.at[sender],
            device_id={"blk": sender},
            device_id_type=pl.DeviceIdType.MESH,
        ).wait()
        at = pl.ds(own, owned)
        out_total[at, :] = out_total[at, :] + recv[sender].astype(jnp.float32)

    if owned < final.shape[0]:
        final[...] = jnp.zeros_like(final)
    final[0:owned, :] = out_total[pl.ds(own, owned), :]
    out_ref[...] = final[...].T[:, 0:owned].astype(jnp.bfloat16)


def per_device(snapshots, bin_index, positions, directions, taper, beam_order):
    n = lax.axis_size("blk")
    _, local, parts, width = snapshots.shape
    elements, beams = positions.shape[1], directions.shape[1]
    owned = beams // n
    tile_b, tile_e = min(512, beams), min(512, local // 2)

    columns = parts * width
    lanes_last = snapshots[0].transpose(1, 2, 0).reshape(columns, local)
    hbm = pl.BlockSpec(memory_space=pl.ANY)
    vmem = pl.BlockSpec(memory_space=pltpu.VMEM)
    result = pl.pallas_call(
        functools.partial(kernel, n, tile_b, tile_e),
        out_shape=jax.ShapeDtypeStruct((columns, owned), jnp.bfloat16),
        in_specs=[pl.BlockSpec(memory_space=pltpu.SMEM), vmem, hbm, vmem, hbm, vmem],
        out_specs=vmem,
        scratch_shapes=[
            pltpu.VMEM((3, local), jnp.int32),
            pltpu.VMEM((1, local), jnp.float32),
            pltpu.VMEM((8, local), jnp.float32),
            pltpu.VMEM((8 * (beams // LANES), LANES), jnp.float32),
            pltpu.VMEM((beams, FEATURES), jnp.bfloat16),
            pltpu.VMEM((FEATURES, local), jnp.bfloat16),
            pltpu.VMEM((columns, local), jnp.bfloat16),
            pltpu.VMEM((columns, local), jnp.bfloat16),
            pltpu.VMEM((2, tile_b, tile_e), jnp.float32),
            pltpu.VMEM((2, tile_b, tile_e), jnp.bfloat16),
            pltpu.VMEM((2, tile_b, tile_e), jnp.bfloat16),
            pltpu.VMEM((2, tile_b, columns), jnp.float32),
            pltpu.VMEM((beams, columns), jnp.bfloat16),
            pltpu.VMEM((n, owned, columns), jnp.bfloat16),
            pltpu.VMEM((max(owned, LANES), columns), jnp.float32),
            pltpu.SemaphoreType.DMA((2,)),
            pltpu.SemaphoreType.DMA((n,)),
            pltpu.SemaphoreType.DMA((n,)),
        ],
        compiler_params=pltpu.CompilerParams(collective_id=0, has_side_effects=True),
    )(
        bin_index, lanes_last, positions, directions,
        taper.reshape(1, elements), beam_order.reshape(1, beams),
    )
    return result.reshape(1, parts, width, owned).transpose(3, 0, 1, 2)


def solution(mesh):
    in_specs = (P("groups", "blk", None, None), P("groups"), P(), P(), P(), P())
    out_specs = P("blk", "groups", None, None)
    return jax.shard_map(
        per_device, mesh=mesh, in_specs=in_specs, out_specs=out_specs, check_vma=False
    )
```
